128 devices in a mesh: row: 64 (over y, x, z_hi, core), col: 2 (over z_lo).
Axes of the slice: x: 4, y: 4, z: 4 (z_hi: 2, z_lo: 2; z = z_hi * 2 + z_lo), core: 2. Of those that a mesh axis runs over, the one named last changes fastest.
Arguments:
- tokens: bfloat16 [1024, 8192], P('row', 'col'), may hold values from -6 to 6
- norm_gain: float32 [8192], P('col'), may hold values from 0.1 to 1.9
- gate_weight: bfloat16 [8192, 28672], P('col', 'row'), may hold values from -0.0625 to 0.0625
- up_weight: bfloat16 [8192, 28672], P('col', 'row'), may hold values from -0.0625 to 0.0625
- down_weight: bfloat16 [28672, 8192], P('row', 'col'), may hold values from -0.03125 to 0.03125
Outputs:
- mixed: bfloat16 [1024, 8192], P('row', 'col')
The draws below stay inside these ranges and needn't reach their ends.
All inputs are finite; a program needn't handle non-finite values.
Results may differ from the reference program's by a relative error of at most 0.0065.
Values may be sent and summed in bfloat16 or wider, within the bound.
A program may use at most 128 MiB of HBM per device.

```python
import jax
import jax.numpy as jnp
from jax import lax

D = 8192
FF = 28672
TOKENS = 1024


def block_levels(rng, dims, shards, smallest, largest):
    def one(position, parts):
        heights = jax.random.uniform(jax.random.fold_in(jax.random.fold_in(rng, 6), position), (parts,), jnp.float32, smallest / len(shards), largest / len(shards))
        return jnp.repeat(jnp.exp(heights), dims[position] // parts).reshape((-1,) + (1,) * (len(dims) - position - 1))

    level = one(*shards[0])
    for cut in shards[1:]:
        level = level * one(*cut)
    return level


def centred(stream_key, extent, deviation, reach, cuts=(), held_as=jnp.bfloat16):
    array = jax.random.normal(stream_key, extent, jnp.float32) * deviation
    if len(cuts) > 0:
        array = block_levels(stream_key, extent, cuts, -0.22, 0.18) * array
    return jnp.clip(array, min=-reach, max=reach).astype(held_as)


def setup_inputs(seed: int = 0) -> dict:
    seeds = jax.random.split(jax.random.key(seed), 6)
    tokens = centred(seeds[0], (TOKENS, D), 1.0, 6.0, ((0, 64), (1, 2)))
    norm_gain = jnp.clip(1.0 + 0.18 * jax.random.normal(seeds[1], (D,), jnp.float32), 0.1, 1.9)
    gate_weight = centred(seeds[2], (D, FF), D ** -0.5, 0.0625, ((0, 2), (1, 64)))
    up_weight = centred(seeds[3], (D, FF), D ** -0.5, 0.0625, ((0, 2), (1, 64)))
    down_weight = centred(seeds[4], (FF, D), FF ** -0.5, 0.03125, ((0, 64), (1, 2)))
    return dict(tokens=tokens, norm_gain=norm_gain, gate_weight=gate_weight, up_weight=up_weight, down_weight=down_weight)


def reference(tokens, norm_gain, gate_weight, up_weight, down_weight):
    widened = tokens.astype(jnp.float32)
    squares = lax.optimization_barrier(jnp.sum(widened * widened, axis=1, keepdims=True))
    normed = (widened * norm_gain[None, :] / jnp.sqrt(squares / D + 1e-05)).astype(jnp.bfloat16)
    gate = jnp.dot(normed, gate_weight, preferred_element_type=jnp.float32)
    up = jnp.dot(normed, up_weight, preferred_element_type=jnp.float32)
    hidden = (jax.nn.silu(gate) * up).astype(jnp.bfloat16)
    return jnp.dot(hidden, down_weight, preferred_element_type=jnp.float32).astype(jnp.bfloat16)
```

```python
import jax
import jax.numpy as jnp
from jax import lax
from jax.experimental import pallas as pl
from jax.experimental.pallas import tpu as pltpu
from jax.sharding import PartitionSpec as P

D = 8192
BF = jnp.bfloat16
F32 = jnp.float32
MESH = pl.DeviceIdType.MESH
CHUNKS = 4
EARLY, LATE = 0, 1


def layer(tok, gain, wg, wu, wd, out, x, wgu, wdn, tokv, tokp, gainv, sq, sqr,
          acc, bsend, brecv, hid, psend, precv, pown, part, rxa, ta, ua, rxb, tb,
          fown, zsend, zrecv, osend, orecv,
          loc, pre_s, pre_r, ag_s, ag_r, za_s, za_r, fw_s, fw_r, b_s, b_r, c_s, c_r,
          p_s, p_r, ra_s, ra_r, rb_s, rb_r, zr_s, zr_r, o_s, o_r):
    me = lax.axis_index("row")
    c = lax.axis_index("col")
    core = me % 2
    zh = (me // 2) % 2
    xx = (me // 4) % 4
    yy = me // 16
    other = 1 - core

    def row_at(y, x_, z, k):
        return ((y * 4 + x_) * 2 + z) * 2 + k

    mate = {"row": row_at(yy, xx, zh, other), "col": c}
    pair = {"row": me, "col": 1 - c}
    pair_mate = {"row": row_at(yy, xx, zh, other), "col": 1 - c}
    far = {"row": row_at(yy, xx, 1 - zh, core), "col": c}
    xs = tuple({"row": row_at(yy, (xx + d) % 4, zh, core), "col": c} for d in (3, 1))
    ys = tuple({"row": row_at((yy + d) % 4, xx, zh, core), "col": c} for d in (3, 1))

    pending = []

    def send(src, dst, ssem, rsem, to):
        copy = pltpu.make_async_remote_copy(
            src_ref=src, dst_ref=dst, send_sem=ssem, recv_sem=rsem,
            device_id=to, device_id_type=MESH)
        copy.start()
        pending.append(copy)

    def arrived(dst, ssem, rsem, frm):
        pltpu.make_async_remote_copy(
            src_ref=dst, dst_ref=dst, send_sem=ssem, recv_sem=rsem,
            device_id=frm, device_id_type=MESH).wait_recv()

    tok_in = [pltpu.make_async_copy(tok.at[:, pl.ds(1024 * q, 1024)], tokv.at[q], loc.at[q]) for q in range(4)]
    gain_in = [pltpu.make_async_copy(gain.at[:, pl.ds(1024 * q, 1024)], gainv.at[q], loc.at[4 + q]) for q in range(4)]
    w_in = [pltpu.make_async_copy(wg, wgu.at[0], loc.at[8]),
            pltpu.make_async_copy(wu, wgu.at[1], loc.at[9])]
    w_in += [pltpu.make_async_copy(wd.at[:, pl.ds(1024 * q, 1024)], wdn.at[q], loc.at[10 + q]) for q in range(4)]
    for copy in tok_in + gain_in + w_in:
        copy.start()

    barrier = pltpu.get_barrier_semaphore()
    friends = (mate, pair, pair_mate, far) + xs + ys
    for friend in friends:
        pl.semaphore_signal(barrier, inc=1, device_id=friend, device_id_type=MESH)

    for copy in tok_in:
        copy.wait()
    total = jnp.zeros((16, 128), F32)
    for q in range(4):
        for i in range(8):
            v = tokv[q, :, 128 * i:128 * i + 128].astype(F32)
            total = total + v * v
    sq[...] = total

    pl.semaphore_wait(barrier, len(friends))

    send(sq, sqr.at[0], pre_s.at[0], pre_r.at[0], mate)
    send(sq, sqr.at[1], pre_s.at[1], pre_r.at[1], pair)
    send(sq, sqr.at[2], pre_s.at[2], pre_r.at[2], pair_mate)
    send(tokv.at[pl.ds(2 * other, 2)], tokp, pre_s.at[3], pre_r.at[3], mate)
    for copy in gain_in:
        copy.wait()
    arrived(sqr.at[1], pre_s.at[1], pre_r.at[1], pair)
    inv_own = 1.0 / jnp.sqrt(jnp.sum(sq[...] + sqr[1], axis=1, keepdims=True) / D + 1e-05)
    for s in range(2):
        q = 2 * core + s
        x[q, core, yy, xx] = (tokv[q].astype(F32) * gainv[q] * inv_own).astype(BF)
    arrived(sqr.at[0], pre_s.at[0], pre_r.at[0], mate)
    arrived(sqr.at[2], pre_s.at[2], pre_r.at[2], pair_mate)
    arrived(tokp, pre_s.at[3], pre_r.at[3], mate)
    inv_mate = 1.0 / jnp.sqrt(jnp.sum(sqr[0] + sqr[2], axis=1, keepdims=True) / D + 1e-05)
    for s in range(2):
        q = 2 * core + s
        x[q, other, yy, xx] = (tokp[s].astype(F32) * gainv[q] * inv_mate).astype(BF)

    first = (xs, ys)
    second = (ys, xs)
    pcoord = (xx, yy)
    rcoord = (yy, xx)

    def rows_of(ref, s, r):
        return ref.at[r] if s == 0 else ref.at[:, r]

    def xblock(j, s, p):
        return x.at[2 * core + s, j, yy, p] if s == 0 else x.at[2 * core + s, j, p, xx]

    def xrow(j, s, r):
        return rows_of(x.at[2 * core + s, j], s, r)

    def forward(j, s, d):
        r = (rcoord[s] + d) % 4
        send(xrow(j, s, r), xrow(j, s, r), fw_s.at[j, s, d], fw_r.at[j, s, d], mate)

    def forwarded(j):
        for s in range(2):
            for d in range(4):
                q = 2 * other + s
                r = (rcoord[s] + d) % 4
                arrived(rows_of(x.at[q, j], s, r), fw_s.at[j, s, d], fw_r.at[j, s, d], mate)

    def cols(ref, h):
        return ref.at[..., pl.ds(512 * h, 512)]

    def g_start(view, j, s, base, here, to):
        send(view(j, s, here), view(j, s, here), ag_s.at[j, s, base], ag_r.at[j, s, base], to[1])
        send(view(j, s, here), view(j, s, here), ag_s.at[j, s, base + 1], ag_r.at[j, s, base + 1], to[0])

    def g_relay(view, j, s, base, here, to):
        low, high = (here + 3) % 4, (here + 1) % 4
        arrived(view(j, s, low), ag_s.at[j, s, base], ag_r.at[j, s, base], to[0])
        send(cols(view(j, s, low), 0), cols(view(j, s, low), 0),
             ag_s.at[j, s, base + 2], ag_r.at[j, s, base + 2], to[1])
        arrived(view(j, s, high), ag_s.at[j, s, base + 1], ag_r.at[j, s, base + 1], to[1])
        send(cols(view(j, s, high), 1), cols(view(j, s, high), 1),
             ag_s.at[j, s, base + 3], ag_r.at[j, s, base + 3], to[0])

    def g_last(view, j, s, base, here, to):
        opp = (here + 2) % 4
        arrived(cols(view(j, s, opp), 0), ag_s.at[j, s, base + 2], ag_r.at[j, s, base + 2], to[0])
        arrived(cols(view(j, s, opp), 1), ag_s.at[j, s, base + 3], ag_r.at[j, s, base + 3], to[1])

    def a1(j):
        for s in range(2):
            g_start(xblock, j, s, 0, pcoord[s], first[s])

    def a2(j):
        for s in range(2):
            g_relay(xblock, j, s, 0, pcoord[s], first[s])

    def a3(j):
        for s in range(2):
            g_last(xblock, j, s, 0, pcoord[s], first[s])
            g_start(xrow, j, s, 4, rcoord[s], second[s])
            forward(j, s, 0)

    def a4(j):
        for s in range(2):
            g_relay(xrow, j, s, 4, rcoord[s], second[s])
            forward(j, s, 3)
            forward(j, s, 1)

    def a5(j):
        for s in range(2):
            g_last(xrow, j, s, 4, rcoord[s], second[s])
            forward(j, s, 2)

    def zblock(j):
        return x.at[pl.ds(2 * core, 2), j, yy, xx]

    def z_start():
        for j in range(2):
            send(zblock(j), zblock(j + 2), za_s.at[j], za_r.at[j], far)

    def z_wait(j):
        arrived(zblock(j), za_s.at[j - 2], za_r.at[j - 2], far)

    weights_waited = []

    def m1(j):
        if not weights_waited:
            w_in[0].wait()
            w_in[1].wait()
            weights_waited.append(1)
        forwarded(j)

        @pl.loop(0, 2)
        def _(g):
            t = None
            for q in range(4):
                y_ = jnp.dot(x[q, j].reshape(256, 1024), wgu[g, 1024 * q:1024 * q + 1024, :],
                             preferred_element_type=F32)
                t = y_ if t is None else t + y_
            acc[j, g] = t.reshape(2, 128, 448)
            bsend[j, g] = acc[j, g, 1 - c].astype(BF)
            pltpu.make_async_remote_copy(
                src_ref=bsend.at[j, g], dst_ref=brecv.at[j, g], send_sem=b_s.at[j, g],
                recv_sem=b_r.at[j, g], device_id=pair, device_id_type=MESH).start()

        for g in range(2):
            pending.append(pltpu.make_async_remote_copy(
                src_ref=bsend.at[j, g], dst_ref=brecv.at[j, g], send_sem=b_s.at[j, g],
                recv_sem=b_r.at[j, g], device_id=pair, device_id_type=MESH))

    def hidden(j):
        for g in range(2):
            arrived(brecv.at[j, g], b_s.at[j, g], b_r.at[j, g], pair)
        gate = acc[j, 0, c] + brecv[j, 0].astype(F32)
        up = acc[j, 1, c] + brecv[j, 1].astype(F32)
        hid[j, c] = (gate / (1.0 + jnp.exp(-gate)) * up).astype(BF)
        send(hid.at[j, c], hid.at[j, c], c_s.at[j], c_r.at[j], pair)

    def m2(j):
        if len(weights_waited) == 1:
            for copy in w_in[2:]:
                copy.wait()
            weights_waited.append(1)
        arrived(hid.at[j, 1 - c], c_s.at[j], c_r.at[j], pair)
        for s in range(2):
            h = hid[j].reshape(256, 448)
            psend[j, s] = jnp.dot(h, wdn[2 * other + s], preferred_element_type=F32).astype(BF)
            send(psend.at[j, s], precv.at[j, s], p_s.at[j, s], p_r.at[j, s], mate)

        @pl.loop(0, 2)
        def _(s):
            h = hid[j].reshape(256, 448)
            pown[s] = jnp.dot(h, wdn[2 * core + s], preferred_element_type=F32)

        for s in range(2):
            arrived(precv.at[j, s], p_s.at[j, s], p_r.at[j, s], mate)

            @pl.loop(0, 4)
            def _(r):
                at = pl.ds(pl.multiple_of(64 * r, 64), 64)
                part[j, s, r] = (pown[s, at, :] + precv[j, s, at, :].astype(F32)).astype(BF).reshape(4, 16, 1024)
        r1(part.at[j], j, 0, rxa, ra_s, ra_r, rcoord, second, True)

    def piece(ref, s, r, byrow):
        if not byrow:
            return ref.at[s, r]
        return ref.at[s, r] if s == 0 else ref.at[s, :, r]

    def r1(src, j, base, rx, ss, rs, coord, to, byrow):
        for s in range(2):
            here = coord[s]
            lo, hi, op = (here + 3) % 4, (here + 1) % 4, (here + 2) % 4
            up_, down = to[s][1], to[s][0]
            for slot, which, h, dev in ((0, op, 0, up_), (3, op, 1, down), (1, hi, 1, up_), (4, lo, 0, down)):
                send(cols(piece(src, s, which, byrow), h), rx.at[j, s, slot],
                     ss.at[j, s, slot], rs.at[j, s, slot], dev)

    def r2(src, j, rx, t, ss, rs, coord, to, byrow):
        for s in range(2):
            here = coord[s]
            lo, hi = (here + 3) % 4, (here + 1) % 4
            up_, down = to[s][1], to[s][0]
            for slot, which, h, k, frm, dev in ((0, hi, 0, 2, down, up_), (3, lo, 1, 5, up_, down)):
                arrived(rx.at[j, s, slot], ss.at[j, s, slot], rs.at[j, s, slot], frm)
                own = cols(piece(src, s, which, byrow), h)[...].astype(F32)
                t[j, s, h] = (own + rx[j, s, slot].astype(F32)).astype(BF)
                send(t.at[j, s, h], rx.at[j, s, k], ss.at[j, s, k], rs.at[j, s, k], dev)

    def r3(src, j, rx, ss, rs, coord, to, byrow, s, put):
        here = coord[s]
        for k, frm in ((1, 0), (2, 0), (4, 1), (5, 1)):
            arrived(rx.at[j, s, k], ss.at[j, s, k], rs.at[j, s, k], to[s][frm])
        for h, (a, b) in enumerate(((2, 4), (1, 5))):
            own = cols(piece(src, s, here, byrow), h)[...].astype(F32)
            put(h, own + rx[j, s, a].astype(F32) + rx[j, s, b].astype(F32))

    def ra2(j):
        r2(part.at[j], j, rxa, ta, ra_s, ra_r, rcoord, second, True)

    def ra3(j):
        for s in range(2):
            def put(h, v, s=s):
                ua[j, s, :, :, 512 * h:512 * h + 512] = v.astype(BF)
            r3(part.at[j], j, rxa, ra_s, ra_r, rcoord, second, True, s, put)
        r1(ua.at[j], j, 0, rxb, rb_s, rb_r, pcoord, first, False)

    def rb2(j):
        r2(ua.at[j], j, rxb, tb, rb_s, rb_r, pcoord, first, False)

    def rb3(j):
        for s in range(2):
            def put(h, v, s=s):
                if j < 2:
                    fown[j, s, :, 512 * h:512 * h + 512] = v
                else:
                    zsend[j - 2, s, :, 512 * h:512 * h + 512] = v.astype(BF)
            r3(ua.at[j], j, rxb, rb_s, rb_r, pcoord, first, False, s, put)
        if j >= 2:
            send(zsend.at[j - 2], zrecv.at[j - 2], zr_s.at[j - 2], zr_r.at[j - 2], far)

    def finish():
        for j in range(2):
            arrived(zrecv.at[j], zr_s.at[j], zr_r.at[j], far)
        osend[...] = (fown[other] + zrecv[other].astype(F32)).astype(BF)
        send(osend, orecv, o_s.at[0], o_r.at[0], mate)
        for s in range(2):
            at = pl.ds(pl.multiple_of((2 * core + s) * 1024, 1024), 1024)
            out[:, at] = (fown[core, s] + zrecv[core, s].astype(F32)).astype(BF)
        arrived(orecv, o_s.at[0], o_r.at[0], mate)
        for s in range(2):
            at = pl.ds(pl.multiple_of((2 * other + s) * 1024, 1024), 1024)
            out[:, at] = orecv[s]

    i0, i1, i2, i3 = 0, 2, 3, 1
    z_start()
    a1(0)
    a1(1)
    a2(0)
    a2(1)
    a3(0)
    z_wait(2)
    z_wait(3)
    a1(2)
    a1(3)
    a4(i0)
    a2(i1)
    a2(i2)
    a3(i1)
    a5(i0)
    m1(i0)
    a3(i2)
    a4(i1)
    a5(i1)
    m1(i1)
    hidden(i0)
    a3(i3)
    a4(i2)
    a5(i2)
    m1(i2)
    hidden(i1)
    a4(i3)
    m2(i0)
    a5(i3)
    m1(i3)
    ra2(i0)
    hidden(i2)
    m2(i1)
    ra3(i0)
    ra2(i1)
    rb2(i0)
    hidden(i3)
    m2(i2)
    ra3(i1)
    rb3(i0)
    ra2(i2)
    rb2(i1)
    m2(i3)
    ra3(i2)
    rb3(i1)
    ra2(i3)
    rb2(i2)
    ra3(i3)
    rb3(i2)
    rb2(i3)
    rb3(i3)
    finish()
    for copy in pending:
        copy.wait_send()


def on_device(tokens, norm_gain, gate_weight, up_weight, down_weight):
    dma = pltpu.SemaphoreType.DMA
    pairs = [(4,), (4, 2, 8), (2,), (4, 2, 4), (4, 2), (4,), (4, 2), (4, 2, 6), (4, 2, 6), (2,), (1,)]
    sems = [dma((14,))]
    for shape in pairs:
        sems += [dma(shape), dma(shape)]
    vm = pltpu.VMEM
    any_ = pl.BlockSpec(memory_space=pl.ANY)
    return pl.pallas_call(
        layer,
        out_shape=jax.ShapeDtypeStruct((16, 4096), BF),
        in_specs=[any_] * 5,
        out_specs=pl.BlockSpec(memory_space=pltpu.VMEM),
        scratch_shapes=[
            vm((4, 4, 4, 4, 16, 1024), BF),
            vm((2, 4096, 448), BF),
            vm((4, 448, 1024), BF),
            vm((4, 16, 1024), BF),
            vm((2, 16, 1024), BF),
            vm((4, 1, 1024), F32),
            vm((16, 128), F32),
            vm((3, 16, 128), F32),
            vm((4, 2, 2, 128, 448), F32),
            vm((4, 2, 128, 448), BF),
            vm((4, 2, 128, 448), BF),
            vm((4, 2, 128, 448), BF),
            vm((4, 2, 256, 1024), BF),
            vm((4, 2, 256, 1024), BF),
            vm((2, 256, 1024), F32),
            vm((4, 2, 4, 4, 16, 1024), BF),
            vm((4, 2, 6, 4, 16, 512), BF),
            vm((4, 2, 2, 4, 16, 512), BF),
            vm((4, 2, 4, 16, 1024), BF),
            vm((4, 2, 6, 16, 512), BF),
            vm((4, 2, 2, 16, 512), BF),
            vm((2, 2, 16, 1024), F32),
            vm((2, 2, 16, 1024), BF),
            vm((2, 2, 16, 1024), BF),
            vm((2, 16, 1024), BF),
            vm((2, 16, 1024), BF),
            *sems,
        ],
        compiler_params=pltpu.CompilerParams(
            collective_id=0, has_side_effects=True, vmem_limit_bytes=62 * 1024 * 1024),
    )(tokens, norm_gain.reshape(1, -1), gate_weight, up_weight, down_weight)


def solution(mesh):
    placed = (P("row", "col"), P("col"), P("col", "row"), P("col", "row"), P("row", "col"))
    return jax.shard_map(
        on_device, mesh=mesh, in_specs=placed, out_specs=P("row", "col"), check_vma=False
    )
```

```python
import jax
import jax.numpy as jnp
from jax import lax
from jax.experimental import pallas as pl
from jax.experimental.pallas import tpu as pltpu
from jax.sharding import PartitionSpec as P

D = 8192
BF = jnp.bfloat16
F32 = jnp.float32
MESH = pl.DeviceIdType.MESH
CHUNKS = 4
EARLY, LATE = 0, 1


def layer(tok, gain, wg, wu, wd, out, x, wgu, wdn, tokv, tokp, gainv, sq, sqr,
          acc, bsend, brecv, hid, psend, precv, pown, part, rxa, ta, ua, rxb, tb,
          fown, zsend, zrecv, osend, orecv,
          loc, pre_s, pre_r, ag_s, ag_r, za_s, za_r, fw_s, fw_r, b_s, b_r, c_s, c_r,
          p_s, p_r, ra_s, ra_r, rb_s, rb_r, zr_s, zr_r, o_s, o_r):
    me = lax.axis_index("row")
    c = lax.axis_index("col")
    core = me % 2
    zh = (me // 2) % 2
    xx = (me // 4) % 4
    yy = me // 16
    other = 1 - core

    def row_at(y, x_, z, k):
        return ((y * 4 + x_) * 2 + z) * 2 + k

    mate = {"row": row_at(yy, xx, zh, other), "col": c}
    pair = {"row": me, "col": 1 - c}
    pair_mate = {"row": row_at(yy, xx, zh, other), "col": 1 - c}
    far = {"row": row_at(yy, xx, 1 - zh, core), "col": c}
    xs = tuple({"row": row_at(yy, (xx + d) % 4, zh, core), "col": c} for d in (3, 1))
    ys = tuple({"row": row_at((yy + d) % 4, xx, zh, core), "col": c} for d in (3, 1))

    pending = []

    def send(src, dst, ssem, rsem, to):
        copy = pltpu.make_async_remote_copy(
            src_ref=src, dst_ref=dst, send_sem=ssem, recv_sem=rsem,
            device_id=to, device_id_type=MESH)
        copy.start()
        pending.append(copy)

    def arrived(dst, ssem, rsem, frm):
        pltpu.make_async_remote_copy(
            src_ref=dst, dst_ref=dst, send_sem=ssem, recv_sem=rsem,
            device_id=frm, device_id_type=MESH).wait_recv()

    tok_in = [pltpu.make_async_copy(tok.at[:, pl.ds(1024 * q, 1024)], tokv.at[q], loc.at[q]) for q in range(4)]
    gain_in = [pltpu.make_async_copy(gain.at[:, pl.ds(1024 * q, 1024)], gainv.at[q], loc.at[4 + q]) for q in range(4)]
    w_in = [pltpu.make_async_copy(wg, wgu.at[0], loc.at[8]),
            pltpu.make_async_copy(wu, wgu.at[1], loc.at[9])]
    w_in += [pltpu.make_async_copy(wd.at[:, pl.ds(1024 * q, 1024)], wdn.at[q], loc.at[10 + q]) for q in range(4)]
    for copy in tok_in + gain_in + w_in:
        copy.start()

    barrier = pltpu.get_barrier_semaphore()
    friends = (mate, pair, pair_mate, far) + xs + ys
    for friend in friends:
        pl.semaphore_signal(barrier, inc=1, device_id=friend, device_id_type=MESH)

    for copy in tok_in:
        copy.wait()
    total = jnp.zeros((16, 128), F32)
    for q in range(4):
        for i in range(8):
            v = tokv[q, :, 128 * i:128 * i + 128].astype(F32)
            total = total + v * v
    sq[...] = total

    pl.semaphore_wait(barrier, len(friends))

    send(sq, sqr.at[0], pre_s.at[0], pre_r.at[0], mate)
    send(sq, sqr.at[1], pre_s.at[1], pre_r.at[1], pair)
    send(sq, sqr.at[2], pre_s.at[2], pre_r.at[2], pair_mate)
    send(tokv.at[pl.ds(2 * other, 2)], tokp, pre_s.at[3], pre_r.at[3], mate)
    for copy in gain_in:
        copy.wait()
    arrived(sqr.at[1], pre_s.at[1], pre_r.at[1], pair)
    inv_own = 1.0 / jnp.sqrt(jnp.sum(sq[...] + sqr[1], axis=1, keepdims=True) / D + 1e-05)
    for s in range(2):
        q = 2 * core + s
        x[q, core, yy, xx] = (tokv[q].astype(F32) * gainv[q] * inv_own).astype(BF)
    arrived(sqr.at[0], pre_s.at[0], pre_r.at[0], mate)
    arrived(sqr.at[2], pre_s.at[2], pre_r.at[2], pair_mate)
    arrived(tokp, pre_s.at[3], pre_r.at[3], mate)
    inv_mate = 1.0 / jnp.sqrt(jnp.sum(sqr[0] + sqr[2], axis=1, keepdims=True) / D + 1e-05)
    for s in range(2):
        q = 2 * core + s
        x[q, other, yy, xx] = (tokp[s].astype(F32) * gainv[q] * inv_mate).astype(BF)

    first = (xs, ys)
    second = (ys, xs)
    pcoord = (xx, yy)
    rcoord = (yy, xx)

    def rows_of(ref, s, r):
        return ref.at[r] if s == 0 else ref.at[:, r]

    def xblock(j, s, p):
        return x.at[2 * core + s, j, yy, p] if s == 0 else x.at[2 * core + s, j, p, xx]

    def xrow(j, s, r):
        return rows_of(x.at[2 * core + s, j], s, r)

    def forward(j, s, d):
        r = (rcoord[s] + d) % 4
        send(xrow(j, s, r), xrow(j, s, r), fw_s.at[j, s, d], fw_r.at[j, s, d], mate)

    def forwarded(j):
        for s in range(2):
            for d in range(4):
                q = 2 * other + s
                r = (rcoord[s] + d) % 4
                arrived(rows_of(x.at[q, j], s, r), fw_s.at[j, s, d], fw_r.at[j, s, d], mate)

    def cols(ref, h):
        return ref.at[..., pl.ds(512 * h, 512)]

    def g_start(view, j, s, base, here, to):
        send(view(j, s, here), view(j, s, here), ag_s.at[j, s, base], ag_r.at[j, s, base], to[1])
        send(view(j, s, here), view(j, s, here), ag_s.at[j, s, base + 1], ag_r.at[j, s, base + 1], to[0])

    def g_relay(view, j, s, base, here, to):
        low, high = (here + 3) % 4, (here + 1) % 4
        arrived(view(j, s, low), ag_s.at[j, s, base], ag_r.at[j, s, base], to[0])
        send(cols(view(j, s, low), 0), cols(view(j, s, low), 0),
             ag_s.at[j, s, base + 2], ag_r.at[j, s, base + 2], to[1])
        arrived(view(j, s, high), ag_s.at[j, s, base + 1], ag_r.at[j, s, base + 1], to[1])
        send(cols(view(j, s, high), 1), cols(view(j, s, high), 1),
             ag_s.at[j, s, base + 3], ag_r.at[j, s, base + 3], to[0])

    def g_last(view, j, s, base, here, to):
        opp = (here + 2) % 4
        arrived(cols(view(j, s, opp), 0), ag_s.at[j, s, base + 2], ag_r.at[j, s, base + 2], to[0])
        arrived(cols(view(j, s, opp), 1), ag_s.at[j, s, base + 3], ag_r.at[j, s, base + 3], to[1])

    def a1(j):
        for s in range(2):
            g_start(xblock, j, s, 0, pcoord[s], first[s])

    def a2(j):
        for s in range(2):
            g_relay(xblock, j, s, 0, pcoord[s], first[s])

    def a3(j):
        for s in range(2):
            g_last(xblock, j, s, 0, pcoord[s], first[s])
            g_start(xrow, j, s, 4, rcoord[s], second[s])
            forward(j, s, 0)

    def a4(j):
        for s in range(2):
            g_relay(xrow, j, s, 4, rcoord[s], second[s])
            forward(j, s, 3)
            forward(j, s, 1)

    def a5(j):
        for s in range(2):
            g_last(xrow, j, s, 4, rcoord[s], second[s])
            forward(j, s, 2)

    def zblock(j):
        return x.at[pl.ds(2 * core, 2), j, yy, xx]

    def z_start():
        for j in range(2):
            send(zblock(j), zblock(j + 2), za_s.at[j], za_r.at[j], far)

    def z_wait(j):
        arrived(zblock(j), za_s.at[j - 2], za_r.at[j - 2], far)

    weights_waited = []

    def m1(j):
        if not weights_waited:
            w_in[0].wait()
            w_in[1].wait()
            weights_waited.append(1)
        forwarded(j)

        @pl.loop(0, 2)
        def _(g):
            t = None
            for q in range(4):
                y_ = lax.dot_general(x[q, j].reshape(256, 1024), wgu[g, :, 1024 * q:1024 * q + 1024],
                                     (((1,), (1,)), ((), ())), preferred_element_type=F32)
                t = y_ if t is None else t + y_
            acc[j, g] = t.reshape(2, 128, 448)
            bsend[j, g] = acc[j, g, 1 - c].astype(BF)
            pltpu.make_async_remote_copy(
                src_ref=bsend.at[j, g], dst_ref=brecv.at[j, g], send_sem=b_s.at[j, g],
                recv_sem=b_r.at[j, g], device_id=pair, device_id_type=MESH).start()

        for g in range(2):
            pending.append(pltpu.make_async_remote_copy(
                src_ref=bsend.at[j, g], dst_ref=brecv.at[j, g], send_sem=b_s.at[j, g],
                recv_sem=b_r.at[j, g], device_id=pair, device_id_type=MESH))

    def hidden(j):
        for g in range(2):
            arrived(brecv.at[j, g], b_s.at[j, g], b_r.at[j, g], pair)
        gate = acc[j, 0, c] + brecv[j, 0].astype(F32)
        up = acc[j, 1, c] + brecv[j, 1].astype(F32)
        hid[j, c] = (gate / (1.0 + jnp.exp(-gate)) * up).astype(BF)
        send(hid.at[j, c], hid.at[j, c], c_s.at[j], c_r.at[j], pair)

    def m2(j):
        if len(weights_waited) == 1:
            for copy in w_in[2:]:
                copy.wait()
            weights_waited.append(1)
        arrived(hid.at[j, 1 - c], c_s.at[j], c_r.at[j], pair)
        for s in range(2):
            h = hid[j].reshape(256, 448)
            psend[j, s] = jnp.dot(h, wdn[2 * other + s], preferred_element_type=F32).astype(BF)
            send(psend.at[j, s], precv.at[j, s], p_s.at[j, s], p_r.at[j, s], mate)

        @pl.loop(0, 2)
        def _(s):
            h = hid[j].reshape(256, 448)
            pown[s] = jnp.dot(h, wdn[2 * core + s], preferred_element_type=F32)

        for s in range(2):
            arrived(precv.at[j, s], p_s.at[j, s], p_r.at[j, s], mate)

            @pl.loop(0, 4)
            def _(r):
                at = pl.ds(pl.multiple_of(64 * r, 64), 64)
                part[j, s, r] = (pown[s, at, :] + precv[j, s, at, :].astype(F32)).astype(BF).reshape(4, 16, 1024)
        r1(part.at[j], j, 0, rxa, ra_s, ra_r, rcoord, second, True)

    def piece(ref, s, r, byrow):
        if not byrow:
            return ref.at[s, r]
        return ref.at[s, r] if s == 0 else ref.at[s, :, r]

    def r1(src, j, base, rx, ss, rs, coord, to, byrow):
        for s in range(2):
            here = coord[s]
            lo, hi, op = (here + 3) % 4, (here + 1) % 4, (here + 2) % 4
            up_, down = to[s][1], to[s][0]
            for slot, which, h, dev in ((0, op, 0, up_), (3, op, 1, down), (1, hi, 1, up_), (4, lo, 0, down)):
                send(cols(piece(src, s, which, byrow), h), rx.at[j, s, slot],
                     ss.at[j, s, slot], rs.at[j, s, slot], dev)

    def r2(src, j, rx, t, ss, rs, coord, to, byrow):
        for s in range(2):
            here = coord[s]
            lo, hi = (here + 3) % 4, (here + 1) % 4
            up_, down = to[s][1], to[s][0]
            for slot, which, h, k, frm, dev in ((0, hi, 0, 2, down, up_), (3, lo, 1, 5, up_, down)):
                arrived(rx.at[j, s, slot], ss.at[j, s, slot], rs.at[j, s, slot], frm)
                own = cols(piece(src, s, which, byrow), h)[...].astype(F32)
                t[j, s, h] = (own + rx[j, s, slot].astype(F32)).astype(BF)
                send(t.at[j, s, h], rx.at[j, s, k], ss.at[j, s, k], rs.at[j, s, k], dev)

    def r3(src, j, rx, ss, rs, coord, to, byrow, s, put):
        here = coord[s]
        for k, frm in ((1, 0), (2, 0), (4, 1), (5, 1)):
            arrived(rx.at[j, s, k], ss.at[j, s, k], rs.at[j, s, k], to[s][frm])
        for h, (a, b) in enumerate(((2, 4), (1, 5))):
            own = cols(piece(src, s, here, byrow), h)[...].astype(F32)
            put(h, own + rx[j, s, a].astype(F32) + rx[j, s, b].astype(F32))

    def ra2(j):
        r2(part.at[j], j, rxa, ta, ra_s, ra_r, rcoord, second, True)

    def ra3(j):
        for s in range(2):
            def put(h, v, s=s):
                ua[j, s, :, :, 512 * h:512 * h + 512] = v.astype(BF)
            r3(part.at[j], j, rxa, ra_s, ra_r, rcoord, second, True, s, put)
        r1(ua.at[j], j, 0, rxb, rb_s, rb_r, pcoord, first, False)

    def rb2(j):
        r2(ua.at[j], j, rxb, tb, rb_s, rb_r, pcoord, first, False)

    def rb3(j):
        for s in range(2):
            def put(h, v, s=s):
                if j < 2:
                    fown[j, s, :, 512 * h:512 * h + 512] = v
                else:
                    zsend[j - 2, s, :, 512 * h:512 * h + 512] = v.astype(BF)
            r3(ua.at[j], j, rxb, rb_s, rb_r, pcoord, first, False, s, put)
        if j >= 2:
            send(zsend.at[j - 2], zrecv.at[j - 2], zr_s.at[j - 2], zr_r.at[j - 2], far)

    def finish():
        for j in range(2):
            arrived(zrecv.at[j], zr_s.at[j], zr_r.at[j], far)
        osend[...] = (fown[other] + zrecv[other].astype(F32)).astype(BF)
        send(osend, orecv, o_s.at[0], o_r.at[0], mate)
        for s in range(2):
            at = pl.ds(pl.multiple_of((2 * core + s) * 1024, 1024), 1024)
            out[:, at] = (fown[core, s] + zrecv[core, s].astype(F32)).astype(BF)
        arrived(orecv, o_s.at[0], o_r.at[0], mate)
        for s in range(2):
            at = pl.ds(pl.multiple_of((2 * other + s) * 1024, 1024), 1024)
            out[:, at] = orecv[s]

    i0, i1, i2, i3 = 0, 2, 3, 1
    z_start()
    a1(0)
    a1(1)
    a2(0)
    a2(1)
    a3(0)
    z_wait(2)
    z_wait(3)
    a1(2)
    a1(3)
    a4(i0)
    a2(i1)
    a2(i2)
    a3(i1)
    a5(i0)
    m1(i0)
    a3(i2)
    a4(i1)
    a5(i1)
    m1(i1)
    hidden(i0)
    a3(i3)
    a4(i2)
    a5(i2)
    m1(i2)
    hidden(i1)
    a4(i3)
    m2(i0)
    a5(i3)
    m1(i3)
    ra2(i0)
    hidden(i2)
    m2(i1)
    ra3(i0)
    ra2(i1)
    rb2(i0)
    hidden(i3)
    m2(i2)
    ra3(i1)
    rb3(i0)
    ra2(i2)
    rb2(i1)
    m2(i3)
    ra3(i2)
    rb3(i1)
    ra2(i3)
    rb2(i2)
    ra3(i3)
    rb3(i2)
    rb2(i3)
    rb3(i3)
    finish()
    for copy in pending:
        copy.wait_send()


def on_device(tokens, norm_gain, gate_weight, up_weight, down_weight):
    dma = pltpu.SemaphoreType.DMA
    pairs = [(4,), (4, 2, 8), (2,), (4, 2, 4), (4, 2), (4,), (4, 2), (4, 2, 6), (4, 2, 6), (2,), (1,)]
    sems = [dma((14,))]
    for shape in pairs:
        sems += [dma(shape), dma(shape)]
    vm = pltpu.VMEM
    any_ = pl.BlockSpec(memory_space=pl.ANY)
    return pl.pallas_call(
        layer,
        out_shape=jax.ShapeDtypeStruct((16, 4096), BF),
        in_specs=[any_] * 5,
        out_specs=pl.BlockSpec(memory_space=pltpu.VMEM),
        scratch_shapes=[
            vm((4, 4, 4, 4, 16, 1024), BF),
            vm((2, 448, 4096), BF),
            vm((4, 448, 1024), BF),
            vm((4, 16, 1024), BF),
            vm((2, 16, 1024), BF),
            vm((4, 1, 1024), F32),
            vm((16, 128), F32),
            vm((3, 16, 128), F32),
            vm((4, 2, 2, 128, 448), F32),
            vm((4, 2, 128, 448), BF),
            vm((4, 2, 128, 448), BF),
            vm((4, 2, 128, 448), BF),
            vm((4, 2, 256, 1024), BF),
            vm((4, 2, 256, 1024), BF),
            vm((2, 256, 1024), F32),
            vm((4, 2, 4, 4, 16, 1024), BF),
            vm((4, 2, 6, 4, 16, 512), BF),
            vm((4, 2, 2, 4, 16, 512), BF),
            vm((4, 2, 4, 16, 1024), BF),
            vm((4, 2, 6, 16, 512), BF),
            vm((4, 2, 2, 16, 512), BF),
            vm((2, 2, 16, 1024), F32),
            vm((2, 2, 16, 1024), BF),
            vm((2, 2, 16, 1024), BF),
            vm((2, 16, 1024), BF),
            vm((2, 16, 1024), BF),
            *sems,
        ],
        compiler_params=pltpu.CompilerParams(
            collective_id=0, has_side_effects=True, vmem_limit_bytes=62 * 1024 * 1024),
    )(tokens, norm_gain.reshape(1, -1), gate_weight.T, up_weight.T, down_weight)


def solution(mesh):
    placed = (P("row", "col"), P("col"), P("col", "row"), P("col", "row"), P("row", "col"))
    return jax.shard_map(
        on_device, mesh=mesh, in_specs=placed, out_specs=P("row", "col"), check_vma=False
    )
```
